32 devices in a mesh: grp: 4 (over z), row: 8 (over y, x, core).
Axes of the slice: x: 2, y: 2, z: 4, core: 2. Of those that a mesh axis runs over, the one named last changes fastest.
Arguments:
- expert_grams: float32 [4, 4096, 4096], P(None, 'row'), may hold values from -32 to 48, as said below
- expert_weights: bfloat16 [4, 4096, 512], P(None, 'row', 'grp'), may hold values from -6 to 6
Outputs:
- merged: float32 [4096, 512], P('row', 'grp')
- residual_ratio: float32 [], replicated
The draws below stay inside these ranges and needn't reach their ends.
Inputs may be any that keep to these rules, and one draw needn't show every extreme that they name: Each expert_grams[k] is exactly symmetric and positive definite.
All inputs are finite; a program needn't handle non-finite values.
Results may differ from the reference program's by a relative error of at most 0.0003.
Values may be sent and summed in bfloat16 or wider, within the bound.
No kernel may reach another device: no remote copies, remote signals or barrier semaphores. Data moves between devices by JAX's collectives and lax.ppermute only.
A program may use at most 128 MiB of HBM per device.

```python
import jax
import jax.numpy as jnp
from jax import lax

D = 4096
EXPERTS = 4
ITERS = 4
COLS = 512


def one_gram(key, expert_index):
    expert_key = jax.random.fold_in(key, 7919 + expert_index)
    sample_key, diagonal_key, common_key = jax.random.split(expert_key, 3)
    samples = D // 8
    samples_matrix = jnp.clip(jax.random.normal(sample_key, (samples, D), jnp.float32), -4.0, 4.0)
    diagonal = jnp.exp(jax.random.uniform(diagonal_key, (D,), jnp.float32, jnp.log(0.05), 0.0))
    raw_gram = jnp.dot(samples_matrix.T, samples_matrix, precision=lax.Precision.HIGHEST) / samples
    return 0.5 * (raw_gram + raw_gram.T) + jnp.diag(diagonal)


def draw_expert_grams(key, part):
    stacked = jnp.stack([one_gram(key, expert) for expert in range(EXPERTS)])
    return stacked.astype(jnp.float32)


def shard_levels(rng, shape, shards, least, high):
    factor_of = 1.0
    for axis_at, blocks in shards:
        steps = jax.random.uniform(jax.random.fold_in(jax.random.fold_in(rng, 6), axis_at), (blocks,), jnp.float32, least / len(shards), high / len(shards))
        factor_of = factor_of * jnp.repeat(jnp.exp(steps), shape[axis_at] // blocks).reshape((-1,) + (1,) * (len(shape) - 1 - axis_at))
    return factor_of


def bell_draw(own_key, extent, width, limit, cuts=(), kind=jnp.bfloat16):
    values = width * jax.random.normal(own_key, extent, jnp.float32)
    if cuts:
        values = values * shard_levels(own_key, extent, cuts, -0.22, 0.18)
    return jnp.clip(values, -limit, limit).astype(kind)


def setup_inputs(seed: int = 0) -> dict:
    seeds = jax.random.split(jax.random.key(seed), 3)
    expert_grams = draw_expert_grams(jax.random.fold_in(seeds[2], 71), 0)
    expert_weights = bell_draw(seeds[1], (EXPERTS, D, COLS), 1.0, 6.0, ((1, 8), (2, 4)))
    return dict(expert_grams=expert_grams, expert_weights=expert_weights)


def reference(expert_grams, expert_weights):
    system = lax.optimization_barrier(jnp.sum(expert_grams, axis=0)) + jnp.eye(D, dtype=jnp.float32)
    target = jnp.zeros((D, COLS), jnp.float32)
    for expert in range(EXPERTS):
        target = target + jnp.dot(expert_grams[expert], expert_weights[expert].astype(jnp.float32), precision=lax.Precision.HIGHEST, preferred_element_type=jnp.float32)
    merged = jnp.zeros((D, COLS), jnp.float32)
    residual = target
    direction = target
    norm_now = lax.optimization_barrier(jnp.sum(residual * residual, axis=0))
    initial = norm_now
    for iteration in range(ITERS):
        mapped = jnp.dot(system, direction, precision=lax.Precision.HIGHEST, preferred_element_type=jnp.float32)
        step_size = norm_now / lax.optimization_barrier(jnp.sum(direction * mapped, axis=0))
        merged = merged + step_size * direction
        residual = residual - step_size * mapped
        norm_next = lax.optimization_barrier(jnp.sum(residual * residual, axis=0))
        direction = residual + norm_next / norm_now * direction
        norm_now = norm_next
    residual_ratio = jnp.sqrt(jnp.sum(norm_now) / jnp.sum(initial))
    return (merged, residual_ratio)
```

```python
import functools

import jax
import jax.numpy as jnp
from jax import lax
from jax.experimental import pallas as pl
from jax.experimental.pallas import tpu as pltpu
from jax.sharding import PartitionSpec as P

ITERS = 4
VMEM = pl.BlockSpec(memory_space=pltpu.VMEM)
F32, BF16 = jnp.float32, jnp.bfloat16


def mixed_bits(size):
    even = [1 << b for b in range(1, size.bit_length() - 1)]
    return even, even[::-1]


def exchange(value, size, even_mask, odd_mask):
    pairs = [(i, i ^ (odd_mask if i & 1 else even_mask)) for i in range(size)]
    return lax.ppermute(value, "row", pairs)


def gather(value, size):
    even, odd = mixed_bits(size)
    slots = [value]
    for e, o in zip(even, odd):
        slots = slots + [exchange(v, size, e, o) for v in slots]
    return slots + [exchange(v, size, 1, 1) for v in slots]


def owners(size):
    me = lax.axis_index("row")
    even, odd = mixed_bits(size)
    masks = [(0, 0)]
    for e, o in zip(even, odd):
        masks = masks + [(a ^ e, b ^ o) for a, b in masks]
    odd_core = me % 2
    near = [me ^ jnp.where(odd_core == 1, b, a) for a, b in masks]
    far = [me ^ 1 ^ jnp.where(odd_core == 1, a, b) for a, b in masks]
    return jnp.stack(near + far).astype(jnp.int32)


def groups(size):
    half = size // 2
    if size == 8:
        return [[0, 4], [1, 2], [5, 6, 3], [7]]
    return [[s, s + half] for s in range(half)]


def split(value):
    high = value.astype(BF16)
    return high, (value - high.astype(F32)).astype(BF16)


def dot(a, b):
    return jnp.dot(a, b, preferred_element_type=F32)


def target_kernel(count, own, fresh, tile, owner, *refs):
    grams = refs[:count]
    weights = refs[count : 2 * count]
    rest = refs[2 * count :]
    if fresh:
        total = None
    else:
        total = rest[0][...]
        rest = rest[1:]
    out, parts = rest[0], rest[1:]
    for j in range(count):
        experts = grams[j].shape[0]
        gram = [grams[j][k] for k in range(experts)]
        system = sum(gram[1:], gram[0])
        if j == own:
            rows = pl.program_id(0) * tile + lax.broadcasted_iota(jnp.int32, system.shape, 0)
            cols = lax.broadcasted_iota(jnp.int32, system.shape, 1)
            system = system + (rows == cols).astype(F32)
        parts[2 * j][...], parts[2 * j + 1][...] = split(system)
        for k in range(experts):
            high, low = split(gram[k])
            part = dot(high, weights[j][k]) + dot(low, weights[j][k])
            total = part if total is None else total + part
    out[...] = total


def target_step(grams, owner, slots, group, total):
    experts, rows, _ = grams.shape
    columns = slots[0].shape[2]
    count = len(group)
    tile = min(rows, 128)

    def gram_spec(slot):
        return pl.BlockSpec((experts, tile, rows), lambda t, o: (0, t, o[slot]))

    row_spec = pl.BlockSpec((tile, columns), lambda t, o: (t, 0))
    part_spec = pl.BlockSpec((tile, rows), lambda t, o: (t, 0))
    weight_spec = pl.BlockSpec((experts, rows, columns), lambda t, o: (0, 0, 0))
    fresh = total is None
    result = pl.pallas_call(
        functools.partial(
            target_kernel, count, group.index(0) if 0 in group else -1, fresh, tile
        ),
        out_shape=[jax.ShapeDtypeStruct((rows, columns), F32)]
        + [jax.ShapeDtypeStruct((rows, rows), BF16)] * (2 * count),
        grid_spec=pltpu.PrefetchScalarGridSpec(
            num_scalar_prefetch=1,
            grid=(rows // tile,),
            in_specs=[gram_spec(s) for s in group]
            + [weight_spec] * count
            + ([] if fresh else [row_spec]),
            out_specs=[row_spec] + [part_spec] * (2 * count),
        ),
        cost_estimate=pl.CostEstimate(
            flops=count * experts * rows * rows * columns * 8,
            bytes_accessed=count * experts * rows * rows * 4,
            transcendentals=0,
        ),
        name="target",
    )(owner, *[grams] * count, *[slots[s] for s in group], *([] if fresh else [total]))
    return result[0], result[1:]


def multiply(high, low, vector):
    if vector.dtype == BF16:
        return dot(high, vector)
    columns = vector.shape[1]
    vector_high, vector_low = split(vector)
    wide = dot(high, jnp.concatenate([vector_high, vector_low], axis=1))
    return wide[:, :columns] + wide[:, columns:] + dot(low, vector_high)


def panel(parts, vectors, total):
    for (high, low), vector in zip(parts, vectors):
        part = multiply(high[...], low[...], vector[...])
        total = part if total is None else total + part
    return total


def pairs_of(refs, count):
    return [(refs[2 * j], refs[2 * j + 1]) for j in range(count)]


def apply_kernel(count, fresh, *refs):
    parts = pairs_of(refs, count)
    vectors = refs[2 * count : 3 * count]
    total = None if fresh else refs[3 * count][...]
    refs[-1][...] = panel(parts, vectors, total)


def cost(count, rows, columns, passes=6):
    return pl.CostEstimate(
        flops=count * rows * rows * columns * passes,
        bytes_accessed=count * rows * rows * 4,
        transcendentals=0,
    )


def apply_step(system, slots, group, total):
    rows, columns = slots[0].shape
    count = len(group)
    operands = [part for s in group for part in system[s]] + [slots[s] for s in group]
    if total is not None:
        operands.append(total)
    return pl.pallas_call(
        functools.partial(apply_kernel, count, total is None),
        out_shape=jax.ShapeDtypeStruct((rows, columns), F32),
        in_specs=[VMEM] * len(operands),
        out_specs=VMEM,
        cost_estimate=cost(count, rows, columns),
        name="apply",
    )(*operands)


def column_sum(value):
    return jnp.sum(value, axis=0, keepdims=True)


def first_kernel(count, size, *refs):
    parts = pairs_of(refs, count)
    vectors = refs[2 * count : 3 * count]
    total, refs = refs[3 * count], refs[3 * count + 1 :]
    slots, (mapped, norm, stacked) = refs[:size], refs[size:]
    mapped[...] = panel(parts, vectors, total[...])
    norm_now = None
    for s in range(size):
        block = slots[s][...]
        stacked[s] = block
        part = column_sum(block * block)
        norm_now = part if norm_now is None else norm_now + part
    norm[...] = norm_now


def first_step(system, slots, group, total):
    rows, columns = slots[0].shape
    size = len(slots)
    operands = [part for s in group for part in system[s]] + [slots[s] for s in group]
    operands += [total] + slots
    return pl.pallas_call(
        functools.partial(first_kernel, len(group), size),
        out_shape=[
            jax.ShapeDtypeStruct((rows, columns), F32),
            jax.ShapeDtypeStruct((1, columns), F32),
            jax.ShapeDtypeStruct((size, rows, columns), F32),
        ],
        in_specs=[VMEM] * len(operands),
        out_specs=[VMEM] * 3,
        cost_estimate=cost(len(group), rows, columns),
        name="first",
    )(*operands)


def update_kernel(count, size, last, *refs):
    parts = pairs_of(refs, count)
    vectors = refs[2 * count : 3 * count]
    refs = refs[3 * count :]
    total, residual, direction, mapped, chained, merged, norm = refs[:7]
    slots, refs = refs[7 : 7 + size], refs[7 + size :]
    product = None
    for s in range(size):
        part = column_sum(direction[s] * slots[s][...].astype(F32))
        product = part if product is None else product + part
    norm_now = norm[...]
    step = norm_now / product
    norm_next = None
    for s in range(size):
        block = residual[s] - step * slots[s][...].astype(F32)
        if not last:
            refs[4][s] = block
        part = column_sum(block * block)
        norm_next = part if norm_next is None else norm_next + part
    scaling = norm_next / norm_now
    chain = chained[...] - step * panel(parts, vectors, total[...])
    mapped_now = mapped[...]
    mapped_next = chain + scaling * mapped_now
    refs[0][...] = mapped_next
    refs[1][...] = merged[...] + step * direction[0]
    refs[2][...] = norm_next
    if last:
        own = residual[0] - step * mapped_now
        own_direction = own + scaling * direction[0]
        refs[3][...] = own
        refs[4][...] = own_direction
        refs[5][0:1] = column_sum(own_direction * mapped_next)
        refs[5][1:2] = column_sum(own * mapped_next)
        refs[5][2:3] = column_sum(mapped_next * mapped_next)
    else:
        refs[3][...] = chain
        for s in range(size):
            refs[5][s] = refs[4][s] + scaling * direction[s]


def update_step(system, slots, group, total, residual, direction, mapped, chained, merged, norm, last):
    size, rows, columns = residual.shape
    operands = [part for s in group for part in system[s]] + [slots[s] for s in group]
    operands += [total, residual, direction, mapped, chained, merged, norm] + slots
    block = jax.ShapeDtypeStruct((rows, columns), F32)
    line = jax.ShapeDtypeStruct((1, columns), F32)
    if last:
        outs = [block, block, line, block, block, jax.ShapeDtypeStruct((3, columns), F32)]
    else:
        whole = jax.ShapeDtypeStruct((size, rows, columns), F32)
        outs = [block, block, line, block, whole, whole]
    return pl.pallas_call(
        functools.partial(update_kernel, len(group), size, last),
        out_shape=outs,
        in_specs=[VMEM] * len(operands),
        out_specs=[VMEM] * len(outs),
        cost_estimate=cost(len(group), rows, columns),
        name="update",
    )(*operands)


def butterfly(value, axis, size):
    bit = 1
    while bit < size:
        value = value + lax.ppermute(value, axis, [(i, i ^ bit) for i in range(size)])
        bit *= 2
    return value


def local(size, planes, expert_grams, expert_weights):
    owner = owners(size)
    order = groups(size)
    slots = gather(expert_weights, size)
    target, system = None, {}
    for group in order:
        target, parts = target_step(expert_grams, owner, slots, group, target)
        for j, s in enumerate(group):
            system[s] = parts[2 * j : 2 * j + 2]

    def partial(slots):
        total = None
        for group in order[:-1]:
            total = apply_step(system, slots, group, total)
        return total

    slots = gather(target, size)
    mapped, norm, residual = first_step(system, slots, order[-1], partial(slots))
    initial = norm
    direction, chained = residual, mapped
    merged = jnp.zeros_like(target)
    for iteration in range(ITERS - 1):
        last = iteration == ITERS - 2
        slots = gather(mapped.astype(BF16) if last else mapped, size)
        total = partial(slots)
        result = update_step(
            system, slots, order[-1], total, residual, direction, mapped, chained, merged, norm, last
        )
        if last:
            mapped, merged, norm, own, own_direction, sums = result
        else:
            mapped, merged, norm, chained, residual, direction = result
    sums = butterfly(sums, "row", size)
    step = norm / sums[0:1]
    merged = merged + step * own_direction
    norm_last = norm - step * (2.0 * sums[1:2] - step * sums[2:3])
    totals = jnp.concatenate(
        [jnp.sum(norm_last, axis=1, keepdims=True), jnp.sum(initial, axis=1, keepdims=True)], axis=1
    )
    totals = butterfly(totals, "grp", planes)
    residual_ratio = jnp.sqrt(totals[0, 0] / totals[0, 1])
    return merged, residual_ratio


def solution(mesh):
    placed = (P(None, "row", None), P(None, "row", "grp"))
    return jax.shard_map(
        functools.partial(local, mesh.shape["row"], mesh.shape["grp"]),
        mesh=mesh,
        in_specs=placed,
        out_specs=(P("row", "grp"), P()),
        check_vma=False,
    )
```

```python
import functools

import jax
import jax.numpy as jnp
from jax import lax
from jax.experimental import pallas as pl
from jax.experimental.pallas import tpu as pltpu
from jax.sharding import PartitionSpec as P

ITERS = 4
VMEM = pl.BlockSpec(memory_space=pltpu.VMEM)
F32, BF16 = jnp.dtype("float32"), jnp.dtype("bfloat16")
EXTRA = {F32: 8, BF16: 16}


def shape(rows, columns, dtype=F32):
    return jax.ShapeDtypeStruct((rows, columns), dtype)


def call(kernel, name, outs, operands, flops=0, aliases=None):
    return pl.pallas_call(
        kernel,
        out_shape=outs,
        in_specs=[VMEM] * len(operands),
        out_specs=[VMEM] * len(outs),
        input_output_aliases=aliases or {},
        cost_estimate=pl.CostEstimate(flops=flops, bytes_accessed=0, transcendentals=0),
        compiler_params=pltpu.CompilerParams(vmem_limit_bytes=8 << 20),
        name=name,
    )(*operands)


def permute(value, axis, size, mask, odd_mask=None):
    odd_mask = mask if odd_mask is None else odd_mask
    return lax.ppermute(value, axis, [(i, i ^ (odd_mask if i & 1 else mask)) for i in range(size)])


def tree(values):
    while len(values) > 1:
        values = [a + b for a, b in zip(values[::2], values[1::2])]
    return values[0]


def masks_of(size):
    even = [1 << b for b in range(1, size.bit_length() - 1)]
    masks = [(0, 0)]
    for e, o in zip(even, even[::-1]):
        masks = masks + [(a ^ e, b ^ o) for a, b in masks]
    return even, even[::-1], masks


def owners(size):
    _, _, masks = masks_of(size)
    me = lax.axis_index("row")
    odd = me % 2 == 1
    near = [me ^ jnp.where(odd, b, a) for a, b in masks]
    far = [me ^ 1 ^ jnp.where(odd, a, b) for a, b in masks]
    return jnp.stack(near + far).astype(jnp.int32)


def gather_with(value, size, step):
    even, odd, _ = masks_of(size)
    half = size // 2
    slots = {0: value, half: permute(value, "row", size, 1)}
    total, ready, width = None, [0, half], 1
    for e, o in zip(even, odd):
        for s in range(width):
            slots[width + s] = permute(slots[s], "row", size, e, o)
        if ready:
            total = step(total, slots, ready)
        new = [slots[width + s] for s in range(width)]
        new, total = lax.optimization_barrier((new, total))
        for s in range(width):
            slots[width + s] = new[s]
            slots[half + width + s] = permute(new[s], "row", size, 1)
        ready = list(range(width, 2 * width))
        width *= 2
    left = [half + s for s in range(1, half // 2)]
    total = step(total, slots, left + ready)
    return total, [slots[s] for s in range(size)], [half + s for s in range(half // 2, half)]


def split(value):
    high = value.astype(BF16)
    return high, (value - high.astype(F32)).astype(BF16)


def dot(a, b):
    return jnp.dot(a, b, preferred_element_type=F32)


def column_sum(value):
    return jnp.sum(value, axis=0, keepdims=True)


def cat(values, axis):
    return values[0] if len(values) == 1 else jnp.concatenate(values, axis=axis)


def target_kernel(count, own, fresh, send, tile, owner, *refs):
    grams, weights, rest = refs[:count], refs[count : 2 * count], refs[2 * count :]
    total = None
    if not fresh:
        total, rest = rest[0][...], rest[1:]
    out, parts = rest[0], rest[1:]
    step = pl.program_id(0)
    for j in range(count):
        experts = grams[j].shape[0]
        gram = [grams[j][k] for k in range(experts)]
        system = tree(gram)
        if j == own:
            rows = step * tile + lax.broadcasted_iota(jnp.int32, system.shape, 0)
            cols = lax.broadcasted_iota(jnp.int32, system.shape, 1)
            system = system + (rows == cols).astype(F32)
        parts[2 * j][...], parts[2 * j + 1][...] = split(system)
        pairs = [split(g) for g in gram]
        left = cat([p[0] for p in pairs] + [p[1] for p in pairs], 1)
        right = [weights[j][k] for k in range(experts)]
        part = dot(left, cat(right + right, 0))
        total = part if total is None else total + part
    if send:
        height = out.shape[0] - EXTRA[F32]
        out[pl.ds(pl.multiple_of(step * tile, tile), tile)] = total
        sums = jnp.broadcast_to(column_sum(total * total), (EXTRA[F32], total.shape[1]))

        @pl.when(step == 0)
        def _():
            out[height:] = sums

        @pl.when(step > 0)
        def _():
            out[height:] += sums
    else:
        out[...] = total


def target_step(grams, owner, system, send, total, slots, group):
    experts, rows, _ = grams.shape
    columns = slots[0].shape[2]
    count = len(group)
    tile = min(rows, 256)
    fresh = total is None

    def gram_spec(slot):
        return pl.BlockSpec((experts, tile, rows), lambda t, o: (0, t, o[slot]))

    row_spec = pl.BlockSpec((tile, columns), lambda t, o: (t, 0))
    out_spec = pl.BlockSpec((rows + EXTRA[F32], columns), lambda t, o: (0, 0)) if send else row_spec
    part_spec = pl.BlockSpec((tile, rows), lambda t, o: (t, 0))
    weight_spec = pl.BlockSpec((experts, rows, columns), lambda t, o: (0, 0, 0))
    own = group.index(0) if 0 in group else -1
    result = pl.pallas_call(
        functools.partial(target_kernel, count, own, fresh, send, tile),
        out_shape=[shape(rows + EXTRA[F32] * send, columns)]
        + [shape(rows, rows, BF16)] * (2 * count),
        grid_spec=pltpu.PrefetchScalarGridSpec(
            num_scalar_prefetch=1,
            grid=(rows // tile,),
            in_specs=[gram_spec(s) for s in group]
            + [weight_spec] * count
            + ([] if fresh else [row_spec]),
            out_specs=[out_spec] + [part_spec] * (2 * count),
        ),
        cost_estimate=pl.CostEstimate(
            flops=count * experts * rows * rows * columns * 8,
            bytes_accessed=count * experts * rows * rows * 4,
            transcendentals=0,
        ),
        compiler_params=pltpu.CompilerParams(vmem_limit_bytes=32 << 20),
        name="target",
    )(owner, *[grams] * count, *[slots[s] for s in group], *([] if fresh else [total]))
    for j, s in enumerate(group):
        system[s] = result[1 + 2 * j : 3 + 2 * j]
    return result[0]


def panel(parts, vectors, total):
    rows = parts[0].shape[0]
    vectors = [v[:rows] for v in vectors]
    high = cat([p[...] for p in parts[::2]], 1)
    if vectors[0].dtype == BF16:
        part = dot(high, cat(vectors, 0))
    else:
        columns = vectors[0].shape[1]
        pairs = [split(v) for v in vectors]
        top = cat([p[0] for p in pairs], 0)
        wide = dot(high, jnp.concatenate([top, cat([p[1] for p in pairs], 0)], axis=1))
        low = cat([p[...] for p in parts[1::2]], 1)
        part = wide[:, :columns] + wide[:, columns:] + dot(low, top)
    return part if total is None else total + part


def apply_kernel(count, fresh, *refs):
    total = None if fresh else refs[3 * count][...]
    refs[-1][...] = panel(refs[: 2 * count], refs[2 * count : 3 * count], total)


def panel_operands(system, slots, group):
    return [part for s in group for part in system[s]] + [slots[s] for s in group]


def apply_step(system, total, slots, group):
    rows = system[0][0].shape[0]
    columns = slots[0].shape[1]
    operands = panel_operands(system, slots, group) + ([] if total is None else [total])
    kernel = functools.partial(apply_kernel, len(group), total is None)
    flops = len(group) * rows * rows * columns * 6
    return call(kernel, "apply", [shape(rows, columns)], operands, flops)[0]


def pack_sums(sums, dtype):
    lines = []
    for value in sums:
        if dtype == F32:
            lines.append(value)
        else:
            high, rest = split(value)
            middle = rest
            low = (value - high.astype(F32) - middle.astype(F32)).astype(BF16)
            lines += [high.astype(F32), middle.astype(F32), low.astype(F32)]
    lines.append(jnp.zeros((EXTRA[dtype] - len(lines), sums[0].shape[1]), F32))
    return jnp.concatenate(lines, axis=0).astype(dtype)


def read_sums(slots, rows, count):
    total = tree([s[rows:].astype(F32) for s in slots])
    if slots[0].dtype == F32:
        return [total[i : i + 1] for i in range(count)]
    return [
        (total[3 * i + 2 : 3 * i + 3] + total[3 * i + 1 : 3 * i + 2]) + total[3 * i : 3 * i + 1]
        for i in range(count)
    ]


def products(residual, direction, mapped):
    return [column_sum(v * mapped) for v in (direction, residual, mapped)]


def first_kernel(count, size, *refs):
    parts, vectors, refs = refs[: 2 * count], refs[2 * count : 3 * count], refs[3 * count :]
    total, slots, (message, norm) = refs[0], refs[1 : 1 + size], refs[1 + size :]
    rows = total.shape[0]
    residual = slots[0][:rows]
    mapped = panel(parts, vectors, total[...])
    message[:rows] = mapped
    message[rows:] = pack_sums(products(residual, residual, mapped), F32)
    (norm[...],) = read_sums(slots, rows, 1)


def first_step(system, total, slots, group):
    rows, columns = total.shape
    operands = panel_operands(system, slots, group) + [total] + slots
    kernel = functools.partial(first_kernel, len(group), len(slots))
    outs = [shape(rows + EXTRA[F32], columns), shape(1, columns)]
    return call(kernel, "first", outs, operands, len(group) * rows * rows * columns * 6)


def update_kernel(count, size, merge, kind, *refs):
    parts, vectors, refs = refs[: 2 * count], refs[2 * count : 3 * count], refs[3 * count :]
    total, residual, direction, mapped, chained, norm, start = refs[:7]
    refs = refs[7:]
    slots, refs = refs[:size], refs[size:]
    if merge:
        merged, refs = refs[0], refs[1:]
    rows = total.shape[0]
    product, cross, square = read_sums(slots, rows, 3)
    norm_now = norm[...]
    step = norm_now / product
    norm_next = jnp.maximum(norm_now - step * (2.0 * cross - step * square), 0.0)
    scaling = norm_next / norm_now
    direction_now, mapped_now = direction[:rows], mapped[:rows]
    residual_next = residual[:rows] - step * mapped_now
    direction_next = residual_next + scaling * direction_now
    chain = chained[:rows] - step * panel(parts, vectors, total[...])
    mapped_next = chain + scaling * mapped_now
    sums = products(residual_next, direction_next, mapped_next)
    refs[0][...] = direction_next
    refs[1][...] = step * direction_now + (merged[...] if merge else 0.0)
    if kind == "end":
        begin = start[:rows]
        sums += [column_sum(residual_next * residual_next), column_sum(begin * begin)]
        refs[2][...] = jnp.concatenate(sums + sums[:3], axis=0)
        return
    refs[2][...] = residual_next
    refs[3][...] = chain
    refs[4][...] = norm_next
    refs[5][:rows] = mapped_next.astype(refs[5].dtype)
    refs[5][rows:] = pack_sums(sums, refs[5].dtype)
    if kind == BF16:
        refs[6][...] = mapped_next


def update_step(system, total, slots, group, state, start, kind):
    rows, columns = total.shape
    residual, direction, mapped, chained, norm, merged = state
    operands = panel_operands(system, slots, group)
    operands += [total, residual, direction, mapped, chained, norm, start] + slots
    if merged is not None:
        operands.append(merged)
    block = shape(rows, columns)
    outs = [block, block]
    if kind == "end":
        outs += [shape(8, columns)]
    else:
        outs += [block, block, shape(1, columns), shape(rows + EXTRA[kind], columns, kind)]
        outs += [block] if kind == BF16 else []
    kernel = functools.partial(update_kernel, len(group), len(slots), merged is not None, kind)
    return call(kernel, "update", outs, operands, len(group) * rows * rows * columns * 6)


def join_kernel(count, *refs):
    refs[-1][...] = tree([r[...] for r in refs[:count]])


def row_sum(value, size):
    others = [permute(value, "row", size, m) for m in range(2, size, 2)]
    values = [value] + others
    kernel = functools.partial(join_kernel, len(values))
    value = call(kernel, "join", [shape(*value.shape)], values)[0]
    return [value, permute(value, "row", size, 1)]


def finish_kernel(near, far, direction, merged, out, totals):
    sums = near[...] + far[...]
    product, cross, square, norm, initial = [sums[i : i + 1] for i in range(5)]
    step = norm / product
    out[...] = merged[...] + step * direction[...]
    norm_last = jnp.maximum(norm - step * (2.0 * cross - step * square), 0.0)
    totals[...] = jnp.concatenate([norm_last, initial] + [norm] * 6, axis=0)


def ratio_kernel(count, *refs):
    total = tree([r[...] for r in refs[:count]])
    total = jnp.sum(total, axis=1, keepdims=True)
    refs[-1][...] = jnp.sqrt(total[0:1] / total[1:2])


def local(size, planes, expert_grams, expert_weights):
    _, rows, _ = expert_grams.shape
    columns = expert_weights.shape[2]
    owner = owners(size)
    system = {}
    block = functools.partial(target_step, expert_grams, owner, system)
    total, slots, group = gather_with(expert_weights, size, functools.partial(block, False))
    target = block(True, total, slots, group)
    apply = functools.partial(apply_step, system)

    total, slots, group = gather_with(target, size, apply)
    message, norm = first_step(system, total, slots, group)
    state = (target, target, message, message, norm, None)
    for iteration in range(ITERS - 1):
        total, slots, group = gather_with(message, size, apply)
        kind = [F32, BF16, "end"][max(0, iteration - ITERS + 4)]
        result = update_step(system, total, slots, group, state, target, kind)
        if kind == "end":
            direction, merged, sums = result
            break
        direction, merged, residual, chained, norm, message = result[:6]
        mapped = result[6] if kind == BF16 else message
        state = (residual, direction, mapped, chained, norm, merged)
    near, far = row_sum(sums, size)
    operands = [near, far, direction, merged]
    merged, totals = call(finish_kernel, "finish", [shape(rows, columns), shape(8, columns)], operands)
    operands = [totals] + [permute(totals, "grp", planes, m) for m in range(1, planes)]
    ratio = call(functools.partial(ratio_kernel, planes), "ratio", [shape(1, 1)], operands)[0]
    return merged, ratio[0, 0]


def solution(mesh):
    placed = (P(None, "row", None), P(None, "row", "grp"))
    return jax.shard_map(
        functools.partial(local, mesh.shape["row"], mesh.shape["grp"]),
        mesh=mesh,
        in_specs=placed,
        out_specs=(P("row", "grp"), P()),
        check_vma=False,
    )
```
